16 devices in a mesh: dp: 4 (over z, y), sh: 4 (over x, core).
Axes of the slice: x: 2, y: 2, z: 2, core: 2. Of those that a mesh axis runs over, the one named last changes fastest.
Arguments:
- k_prefill: bfloat16 [16, 7168, 8, 256], P('dp', None, 'sh'), parts along dimension 0
- v_prefill: bfloat16 [16, 7168, 8, 256], P('dp', None, 'sh'), parts along dimension 0
- lengths: int32 [16], P('dp'), parts along dimension 0
- residual: bfloat16 [16, 3584], P(('dp', 'sh')), parts along dimension 0
- norm_gain: bfloat16 [3584], replicated
- w_query: bfloat16 [3584, 4096], replicated
- w_key: bfloat16 [3584, 2048], replicated
- w_value: bfloat16 [3584, 2048], replicated
- w_out: bfloat16 [4096, 3584], replicated
Outputs:
- output 1: bfloat16 [16, 3584], P(('dp', 'sh')), parts along dimension 0
- output 2: bfloat16 [16, 4096, 8, 256], P(('dp', 'sh')), parts along dimension 0
- output 3: bfloat16 [16, 4096, 8, 256], P(('dp', 'sh')), parts along dimension 0
There are 4 independent parts. The reference program is written for one: setup_inputs(seed, part) draws one part's arguments, and reference() takes and returns one part's arrays. A program takes and returns all parts, laid end to end along the dimension named above; an argument that names none is the same for every part.
All inputs are finite; a program needn't handle non-finite values.
Results may differ from the reference program's by a relative error of at most 0.00415.
Values are sent between devices in bfloat16 or wider.
A program may use at most 1 GiB of HBM per device.

```python
import jax
import jax.numpy as jnp
from jax import lax

MODEL_DIM = 3584
HEADS = 16
KV_HEADS = 8
HEAD_DIM = 256
WINDOW = 4096
SEQ_LEN = 7168
BATCH = 4
Q_GROUP = HEADS // KV_HEADS
Q_WIDTH = HEADS * HEAD_DIM
KV_WIDTH = KV_HEADS * HEAD_DIM
THETA = 10000.0
EPS = 1e-5


def setup_inputs(seed: int = 0, part: int = 0) -> dict:
    root_key = jax.random.key(seed)
    part_root, shared_root = jax.random.split(root_key)
    part_keys = jax.random.split(jax.random.fold_in(part_root, part), 4)
    shared_keys = jax.random.split(shared_root, 5)
    kv_shape = (BATCH, SEQ_LEN, KV_HEADS, HEAD_DIM)
    k_prefill = jax.random.normal(part_keys[0], kv_shape, jnp.float32).astype(jnp.bfloat16)
    v_prefill = jax.random.normal(part_keys[1], kv_shape, jnp.float32).astype(jnp.bfloat16)
    lengths = jax.random.randint(part_keys[2], (BATCH,), 1, SEQ_LEN + 1, dtype=jnp.int32)
    lengths = lengths.at[0].set(SEQ_LEN).at[1].set(1)
    residual = jax.random.normal(part_keys[3], (BATCH, MODEL_DIM), jnp.float32).astype(jnp.bfloat16)
    norm_gain = (1.0 + 0.3 * jax.random.normal(shared_keys[0], (MODEL_DIM,), jnp.float32)).astype(jnp.bfloat16)
    w_query = (jax.random.normal(shared_keys[1], (MODEL_DIM, Q_WIDTH), jnp.float32) * (2.0 / MODEL_DIM ** 0.5)).astype(jnp.bfloat16)
    w_key = (jax.random.normal(shared_keys[2], (MODEL_DIM, KV_WIDTH), jnp.float32) * (3.0 / MODEL_DIM ** 0.5)).astype(jnp.bfloat16)
    w_value = (jax.random.normal(shared_keys[3], (MODEL_DIM, KV_WIDTH), jnp.float32) * (3.0 / MODEL_DIM ** 0.5)).astype(jnp.bfloat16)
    w_out = (jax.random.normal(shared_keys[4], (Q_WIDTH, MODEL_DIM), jnp.float32) * (2.0 / Q_WIDTH ** 0.5)).astype(jnp.bfloat16)
    return {'k_prefill': k_prefill, 'v_prefill': v_prefill, 'lengths': lengths, 'residual': residual, 'norm_gain': norm_gain, 'w_query': w_query, 'w_key': w_key, 'w_value': w_value, 'w_out': w_out}


def rolling_cache(prefill, lengths):
    slot_ids = jnp.arange(WINDOW, dtype=jnp.int32)
    last_pos = lengths[:, None] - 1
    held_pos = last_pos - jnp.remainder(last_pos - slot_ids[None, :], WINDOW)
    held = jax.vmap(lambda row_vals, row_idx: jnp.take(row_vals, row_idx, axis=0))(prefill, jnp.maximum(held_pos, 0))
    return jnp.where((held_pos >= 0)[:, :, None, None], held, jnp.zeros((), prefill.dtype))


def rotate(heads, positions):
    half_dim = HEAD_DIM // 2
    inv_freq = THETA ** (-2.0 * jnp.arange(half_dim, dtype=jnp.float32) / HEAD_DIM)
    angles = positions.astype(jnp.float32).reshape(positions.shape + (1,) * (heads.ndim - 1)) * inv_freq
    cos_part = jnp.cos(angles)
    sin_part = jnp.sin(angles)
    first_half = heads[..., :half_dim].astype(jnp.float32)
    second_half = heads[..., half_dim:].astype(jnp.float32)
    return jnp.concatenate([first_half * cos_part - second_half * sin_part, second_half * cos_part + first_half * sin_part], axis=-1).astype(jnp.bfloat16)


def attend_row(row_args):
    q_row, k_row, v_row, live_row = row_args
    q_grouped = q_row.reshape(KV_HEADS, Q_GROUP, HEAD_DIM).astype(jnp.float32)
    scores = jnp.einsum('kgd,wkd->kgw', q_grouped, k_row.astype(jnp.float32)) / HEAD_DIM ** 0.5
    scores = jnp.where(live_row[None, None, :], scores, -jnp.inf)
    weights = jax.nn.softmax(scores, axis=-1).astype(jnp.bfloat16)
    mixed = jnp.einsum('kgw,wkd->kgd', weights.astype(jnp.float32), v_row.astype(jnp.float32))
    return mixed.astype(jnp.bfloat16).reshape(Q_WIDTH)


def reference(k_prefill, v_prefill, lengths, residual, norm_gain, w_query, w_key, w_value, w_out):
    k_cache = rolling_cache(k_prefill, lengths)
    v_cache = rolling_cache(v_prefill, lengths)
    resid_f32 = residual.astype(jnp.float32)
    inv_rms = lax.rsqrt(jnp.mean(resid_f32 * resid_f32, axis=-1, keepdims=True) + EPS)
    normed = (resid_f32 * inv_rms * norm_gain.astype(jnp.float32)).astype(jnp.bfloat16)
    q_heads = jnp.dot(normed, w_query, preferred_element_type=jnp.float32).astype(jnp.bfloat16).reshape(BATCH, HEADS, HEAD_DIM)
    k_new = jnp.dot(normed, w_key, preferred_element_type=jnp.float32).astype(jnp.bfloat16).reshape(BATCH, KV_HEADS, HEAD_DIM)
    v_new = jnp.dot(normed, w_value, preferred_element_type=jnp.float32).astype(jnp.bfloat16).reshape(BATCH, KV_HEADS, HEAD_DIM)
    q_heads = rotate(q_heads, lengths)
    k_new = rotate(k_new, lengths)
    slot_ids = jnp.arange(WINDOW, dtype=jnp.int32)
    new_slot = (slot_ids[None, :] == (lengths % WINDOW)[:, None])[:, :, None, None]
    k_cache = jnp.where(new_slot, k_new[:, None], k_cache)
    v_cache = jnp.where(new_slot, v_new[:, None], v_cache)
    live_slot = (lengths[:, None] - jnp.remainder(lengths[:, None] - slot_ids[None, :], WINDOW)) >= 0
    attn_out = lax.map(attend_row, (q_heads, k_cache, v_cache, live_slot))
    resid_out = (resid_f32 + jnp.dot(attn_out, w_out, preferred_element_type=jnp.float32)).astype(jnp.bfloat16)
    return (resid_out, k_cache, v_cache)
```

```python
import functools

import jax
import jax.numpy as jnp
from jax import lax
from jax.experimental import pallas as pl
from jax.experimental.pallas import tpu as pltpu
from jax.sharding import PartitionSpec as P


WINDOW = 4096
THETA = 10000.0
EPS = 1e-5
LANES = 128
BLOCK = 256
DEPTH = 4
VMEM_BYTES = 67043328
K_CHUNKS = (512, 1536, 2048)
V_CHUNKS = (2048, 1536, 512)


def build_kernel(pieces, scal_ref, src_ref, _, *refs):
    outs = refs[:len(pieces)]
    buf, other, zeros, in_sem, other_sem, out_sem = refs[len(pieces):]
    me = scal_ref[4]
    last = src_ref.shape[1] - BLOCK
    zeros[...] = jnp.zeros_like(zeros)

    for (j, c0, size), out in zip(pieces, outs):
        row = me ^ j
        length = scal_ref[row]
        wrapped = jnp.maximum(length - WINDOW, 0)
        filled = jnp.minimum(length, WINDOW)
        count = size // BLOCK

        def start_in(i):
            base = c0 + i * BLOCK
            slot = lax.rem(i, DEPTH)
            whole_wrapped = base + BLOCK <= wrapped
            first = jnp.where(whole_wrapped, jnp.minimum(base + WINDOW, last), base)

            @pl.when(base < filled)
            def _():
                pltpu.make_async_copy(src_ref.at[row, pl.ds(first, BLOCK)], buf.at[slot], in_sem.at[slot]).start()

            @pl.when((base < wrapped) & (base + BLOCK > wrapped))
            def _():
                pltpu.make_async_copy(src_ref.at[row, pl.ds(jnp.minimum(base + WINDOW, last), BLOCK)], other, other_sem).start()

        def out_copy(i):
            slot = lax.rem(i, DEPTH)
            return pltpu.make_async_copy(buf.at[slot], out.at[pl.ds(i * BLOCK, BLOCK)], out_sem.at[slot])

        def finish(i):
            base = c0 + i * BLOCK
            slot = lax.rem(i, DEPTH)

            @pl.when(base < filled)
            def _():
                pltpu.make_async_copy(src_ref.at[row, pl.ds(0, BLOCK)], buf.at[slot], in_sem.at[slot]).wait()

                @pl.when((base < wrapped) & (base + BLOCK > wrapped))
                def _():
                    pltpu.make_async_copy(src_ref.at[row, pl.ds(0, BLOCK)], other, other_sem).wait()

                    @pl.loop(0, wrapped - base)
                    def _(s):
                        buf[slot, s] = other[s]

                @pl.when(base + BLOCK > filled)
                def _():
                    @pl.loop(filled - base, BLOCK)
                    def _(s):
                        buf[slot, s] = zeros[0]

                out_copy(i).start()

            @pl.when(base >= filled)
            def _():
                pltpu.make_async_copy(zeros, out.at[pl.ds(i * BLOCK, BLOCK)], out_sem.at[slot]).start()

        for i in range(min(DEPTH - 1, count)):
            start_in(i)

        @pl.loop(0, count)
        def _(i):
            finish(i)
            ahead = i + DEPTH - 1

            @pl.when(ahead < count)
            def _():
                @pl.when(i >= 1)
                def _():
                    out_copy(i - 1).wait()

                start_in(ahead)

        for i in range(max(count - DEPTH, 0), count):
            out_copy(i).wait()


def build(scal, src, pieces, after):
    tile = src.shape[2:]
    return pl.pallas_call(
        functools.partial(build_kernel, pieces),
        out_shape=[jax.ShapeDtypeStruct((size,) + tile, src.dtype) for _, _, size in pieces],
        in_specs=[pl.BlockSpec(memory_space=pltpu.SMEM), pl.BlockSpec(memory_space=pltpu.HBM), pl.BlockSpec(memory_space=pl.ANY)],
        out_specs=[pl.BlockSpec(memory_space=pltpu.HBM)] * len(pieces),
        scratch_shapes=[
            pltpu.VMEM((DEPTH, BLOCK) + tile, src.dtype),
            pltpu.VMEM((BLOCK,) + tile, src.dtype),
            pltpu.VMEM((BLOCK,) + tile, src.dtype),
            pltpu.SemaphoreType.DMA((DEPTH,)),
            pltpu.SemaphoreType.DMA,
            pltpu.SemaphoreType.DMA((DEPTH,)),
        ],
        compiler_params=pltpu.CompilerParams(vmem_limit_bytes=VMEM_BYTES),
        cost_estimate=pl.CostEstimate(flops=10 ** 9, bytes_accessed=sum(p[2] for p in pieces) * 2048, transcendentals=0),
    )(scal, src, after)


def place_kernel(c0, size, has_prev, scal_ref, fresh_ref, own, near, far0, far1, *refs):
    out = refs[1] if has_prev else refs[0]
    buf, in_sem, out_sem = refs[-3:]
    me = scal_ref[4]
    new_slot = lax.rem(scal_ref[me], WINDOW)
    count = size // BLOCK

    def in_copies(i):
        slot = lax.rem(i, DEPTH)
        local = pl.ds(i * BLOCK, BLOCK)
        whole = pl.ds(c0 + i * BLOCK, BLOCK)
        views = (own.at[whole], near.at[whole], far0.at[local], far1.at[local])
        return [
            pltpu.make_async_copy(view, buf.at[slot, :, :, me ^ j], in_sem.at[slot, j])
            for j, view in enumerate(views)
        ]

    def out_copy(i):
        slot = lax.rem(i, DEPTH)
        return pltpu.make_async_copy(buf.at[slot], out.at[pl.ds(c0 + i * BLOCK, BLOCK)], out_sem.at[slot])

    for i in range(min(DEPTH - 1, count)):
        for copy in in_copies(i):
            copy.start()

    @pl.loop(0, count)
    def _(i):
        for copy in in_copies(i):
            copy.wait()
        spot = new_slot - (c0 + i * BLOCK)

        @pl.when((spot >= 0) & (spot < BLOCK))
        def _():
            buf[lax.rem(i, DEPTH), spot] = fresh_ref[...]

        out_copy(i).start()
        ahead = i + DEPTH - 1

        @pl.when(ahead < count)
        def _():
            @pl.when(i >= 1)
            def _():
                out_copy(i - 1).wait()

            for copy in in_copies(ahead):
                copy.start()

    for i in range(max(count - DEPTH, 0), count):
        out_copy(i).wait()


def place(scal, fresh, own, near, far0, far1, c0, prev):
    size = far0.shape[0]
    hbm = pl.BlockSpec(memory_space=pltpu.HBM)
    operands = [scal, fresh, own, near, far0, far1]
    if prev is not None:
        operands.append(prev)
    halves, pair, lanes = own.shape[1:]
    return pl.pallas_call(
        functools.partial(place_kernel, c0, size, prev is not None),
        out_shape=jax.ShapeDtypeStruct((WINDOW, halves, 4, pair, lanes), own.dtype),
        in_specs=[pl.BlockSpec(memory_space=pltpu.SMEM), pl.BlockSpec(memory_space=pltpu.VMEM)] + [hbm] * (len(operands) - 2),
        out_specs=hbm,
        scratch_shapes=[
            pltpu.VMEM((DEPTH, BLOCK, halves, 4, pair, lanes), own.dtype),
            pltpu.SemaphoreType.DMA((DEPTH, 4)),
            pltpu.SemaphoreType.DMA((DEPTH,)),
        ],
        input_output_aliases={} if prev is None else {6: 0},
        compiler_params=pltpu.CompilerParams(vmem_limit_bytes=VMEM_BYTES),
        cost_estimate=pl.CostEstimate(flops=10 ** 9, bytes_accessed=size * 8192, transcendentals=0),
    )(*operands)


def rotate(heads, positions):
    head_dim = heads.shape[-1]
    half_dim = head_dim // 2
    inv_freq = THETA ** (-2.0 * jnp.arange(half_dim, dtype=jnp.float32) / head_dim)
    angles = positions.astype(jnp.float32).reshape(positions.shape + (1,) * (heads.ndim - 1)) * inv_freq
    cos_part = jnp.cos(angles)
    sin_part = jnp.sin(angles)
    first_half = heads[..., :half_dim].astype(jnp.float32)
    second_half = heads[..., half_dim:].astype(jnp.float32)
    return jnp.concatenate([first_half * cos_part - second_half * sin_part, second_half * cos_part + first_half * sin_part], axis=-1).astype(jnp.bfloat16)


def normalize(residual, norm_gain):
    resid_f32 = residual.astype(jnp.float32)
    inv_rms = lax.rsqrt(jnp.mean(resid_f32 * resid_f32, axis=-1, keepdims=True) + EPS)
    return (resid_f32 * inv_rms * norm_gain.astype(jnp.float32)).astype(jnp.bfloat16)


def project(normed, weight):
    return jnp.dot(normed, weight, preferred_element_type=jnp.float32).astype(jnp.bfloat16)


def split_lanes(array):
    halves = array.shape[-1] // LANES
    return jnp.swapaxes(array.reshape(array.shape[:-1] + (halves, LANES)), -3, -2)


def attend_heads(q_heads, k_new, v_new, k_prefill, v_prefill, lengths):
    scale = q_heads.shape[-1] ** 0.5
    positions = jnp.arange(k_prefill.shape[1], dtype=jnp.int32)[None, :]
    live = (positions < lengths[:, None]) & (positions > lengths[:, None] - WINDOW)
    scores = jnp.einsum('rkgd,rwkd->rkgw', q_heads, k_prefill, preferred_element_type=jnp.float32) / scale
    scores = jnp.where(live[:, None, None, :], scores, -jnp.inf)
    new_score = jnp.sum(q_heads.astype(jnp.float32) * k_new.astype(jnp.float32)[:, :, None, :], axis=-1, keepdims=True) / scale
    top = jnp.maximum(jnp.max(scores, axis=-1, keepdims=True), new_score)
    exp_scores = jnp.exp(scores - top)
    new_exp = jnp.exp(new_score - top)
    total = jnp.sum(exp_scores, axis=-1, keepdims=True) + new_exp
    weights = (exp_scores / total).astype(jnp.bfloat16)
    new_weight = (new_exp / total).astype(jnp.bfloat16)
    mixed = jnp.einsum('rkgw,rwkd->rkgd', weights, v_prefill, preferred_element_type=jnp.float32)
    mixed = mixed + new_weight.astype(jnp.float32) * v_new.astype(jnp.float32)[:, :, None, :]
    return mixed.astype(jnp.bfloat16)


def solution(mesh):
    group = mesh.shape['sh']
    head_spec = P('dp', None, 'sh', None)
    row_spec = P(('dp', 'sh'))
    full_spec = P(None, None)

    def swap(array, j):
        return lax.ppermute(array, 'sh', [(i, i ^ j) for i in range(group)])

    def per_device(k_prefill, v_prefill, lengths, residual, norm_gain, w_query, w_key, w_value, w_out):
        kv_heads, head_dim = k_prefill.shape[2:]
        me = lax.axis_index('sh')
        by_row = jnp.arange(group, dtype=jnp.int32) ^ me
        scal = jnp.concatenate([lengths, me[None].astype(jnp.int32)])
        my_length = lax.dynamic_slice_in_dim(lengths, me, 1)

        all_resid = jnp.concatenate([residual] + [swap(residual, j) for j in range(1, group)], axis=0)
        all_resid = jnp.take(all_resid, by_row, axis=0)

        k_src, v_src = split_lanes(k_prefill), split_lanes(v_prefill)

        def far_pieces(chunks):
            starts = [sum(chunks[:i]) for i in range(len(chunks))]
            return [[(2, c0, size), (3, c0, size)] for c0, size in zip(starts, chunks)]

        def send(src, chunks, after):
            far = []
            for pieces in far_pieces(chunks):
                built = build(scal, src, pieces, after)
                far.append([swap(a, p[0]) for a, p in zip(built, pieces)])
                after = built[0]
            own, near = build(scal, src, [(0, 0, WINDOW), (1, 0, WINDOW)], after)
            return own, swap(near, 1), far

        k_own, k_near, k_far = send(k_src, K_CHUNKS, scal)

        normed = normalize(all_resid, norm_gain)
        kv_width = kv_heads * head_dim
        q_width = w_query.shape[1] // group
        q_heads = project(normed, lax.dynamic_slice_in_dim(w_query, me * q_width, q_width, axis=1))
        q_heads = rotate(q_heads.reshape(group, kv_heads, q_width // kv_width, head_dim), lengths)
        k_new = project(normed, lax.dynamic_slice_in_dim(w_key, me * kv_width, kv_width, axis=1))
        v_new = project(normed, lax.dynamic_slice_in_dim(w_value, me * kv_width, kv_width, axis=1))
        k_new = rotate(k_new.reshape(group, kv_heads, head_dim), lengths)
        v_new = v_new.reshape(group, kv_heads, head_dim)
        mixed = attend_heads(q_heads, k_new, v_new, k_prefill, v_prefill, lengths).reshape(group, q_width)
        mixed = jnp.take(mixed, by_row, axis=0)
        mine = [mixed[:1]] + [swap(mixed[j:j + 1], j) for j in range(1, group)]

        v_own, v_near, v_far = send(v_src, V_CHUNKS, mixed)

        attn_out = jnp.take(jnp.concatenate(mine, axis=0), by_row, axis=0).reshape(1, group * q_width)
        resid_out = (residual.astype(jnp.float32) + jnp.dot(attn_out, w_out, preferred_element_type=jnp.float32)).astype(jnp.bfloat16)

        own_normed = normalize(residual, norm_gain)
        k_fresh = rotate(project(own_normed, w_key).reshape(1, group * kv_heads, head_dim), my_length)
        v_fresh = project(own_normed, w_value).reshape(1, group * kv_heads, head_dim)

        def cache(fresh, own, near, far):
            fresh = split_lanes(fresh[0])
            fresh = fresh.reshape(fresh.shape[0], group, kv_heads, LANES)
            out, c0 = None, 0
            for far0, far1 in far:
                out = place(scal, fresh, own, near, far0, far1, c0, out)
                c0 += far0.shape[0]
            return jnp.transpose(out, (0, 2, 3, 1, 4)).reshape(1, WINDOW, group * kv_heads, head_dim)

        return resid_out, cache(k_fresh, k_own, k_near, k_far), cache(v_fresh, v_own, v_near, v_far)

    return jax.shard_map(per_device, mesh=mesh, in_specs=(head_spec, head_spec, P('dp'), P(('dp', 'sh'), None), P(None), full_spec, full_spec, full_spec, full_spec), out_specs=(P(('dp', 'sh'), None), row_spec, row_spec), check_vma=False)
```

```python
import functools
import math

import jax
import jax.numpy as jnp
from jax import lax
from jax.experimental import pallas as pl
from jax.experimental.pallas import tpu as pltpu
from jax.sharding import PartitionSpec as P


WINDOW = 4096
THETA = 10000.0
EPS = 1e-5
LANES = 128
BLOCK = 256
DEPTH = 6
FLIGHT = 16
ZEROS = 32
VMEM_BYTES = 67043328
LOW = 2560
K_CHUNKS = (512, 2048)
V_CHUNKS = (1792, 512, 256)
UNIT = 128
UPPER = (WINDOW - LOW) // UNIT
LANES_OF_CUT = 4
PART = 4


def build_kernel(partners, c0, lens_ref, src_ref, _, *refs):
    ways = len(partners)
    outs = refs[:ways]
    buf, other, in_sem, other_sem, out_sem = refs[ways:]
    me = lax.axis_index('sh')
    size = outs[0].shape[0]
    block = math.gcd(BLOCK, size)
    total = size // block * ways
    last = src_ref.shape[1] - block
    rows = pl.ds(0, block)

    def where(i):
        row = me ^ partners[0]
        for p, j in enumerate(partners[1:]):
            row = jnp.where(lax.rem(i, ways) == p + 1, me ^ j, row)
        return row, c0 + i // ways * block, jnp.maximum(lens_ref[row] - WINDOW, 0)

    def in_copy(i, row, start):
        slot = lax.rem(i, FLIGHT)
        return pltpu.make_async_copy(src_ref.at[row, pl.ds(start, block)], buf.at[slot, rows], in_sem.at[slot])

    def other_copy(row, start):
        return pltpu.make_async_copy(src_ref.at[row, pl.ds(start, block)], other.at[rows], other_sem)

    def out_copy(i, out):
        slot = lax.rem(i, FLIGHT)
        return pltpu.make_async_copy(buf.at[slot, rows], out.at[pl.ds(i // ways * block, block)], out_sem.at[slot])

    def start_in(i):
        row, base, wrapped = where(i)
        in_copy(i, row, jnp.where(base + block <= wrapped, jnp.minimum(base + WINDOW, last), base)).start()

    def finish(i):
        row, base, wrapped = where(i)
        slot = lax.rem(i, FLIGHT)
        in_copy(i, row, 0).wait()

        @pl.when((base < wrapped) & (base + block > wrapped))
        def _():
            copy = other_copy(row, jnp.minimum(base + WINDOW, last))
            copy.start()
            copy.wait()

            @pl.loop(0, wrapped - base)
            def _(s):
                buf[slot, s] = other[s]

        for p, out in enumerate(outs):
            @pl.when(lax.rem(i, ways) == p)
            def _():
                out_copy(i, out).start()

    @pl.loop(0, min(FLIGHT - 1, total))
    def _(i):
        start_in(i)

    @pl.loop(0, total)
    def _(i):
        finish(i)
        ahead = i + FLIGHT - 1

        @pl.when(ahead < total)
        def _():
            @pl.when(i >= 1)
            def _():
                out_copy(i - 1, outs[0]).wait()

            start_in(ahead)

    @pl.loop(max(total - FLIGHT, 0), total)
    def _(i):
        out_copy(i, outs[0]).wait()


def build(lengths, src, partners, c0, size, after):
    tile = src.shape[2:]
    return pl.pallas_call(
        functools.partial(build_kernel, partners, c0),
        out_shape=[jax.ShapeDtypeStruct((size,) + tile, src.dtype) for _ in partners],
        in_specs=[pl.BlockSpec(memory_space=pltpu.SMEM), pl.BlockSpec(memory_space=pltpu.HBM), pl.BlockSpec(memory_space=pl.ANY)],
        out_specs=[pl.BlockSpec(memory_space=pltpu.HBM)] * len(partners),
        scratch_shapes=[
            pltpu.VMEM((FLIGHT, BLOCK) + tile, src.dtype),
            pltpu.VMEM((BLOCK,) + tile, src.dtype),
            pltpu.SemaphoreType.DMA((FLIGHT,)),
            pltpu.SemaphoreType.DMA,
            pltpu.SemaphoreType.DMA((FLIGHT,)),
        ],
        compiler_params=pltpu.CompilerParams(vmem_limit_bytes=VMEM_BYTES),
        cost_estimate=pl.CostEstimate(flops=10 ** 9, bytes_accessed=size * 4096, transcendentals=0),
    )(lengths, src, after)


def place_kernel(c0, size, has_prev, lens_ref, fresh_ref, own, near, far0, far1, *refs):
    out = refs[1] if has_prev else refs[0]
    buf, zeros, in_sem, out_sem = refs[-4:]
    me = lax.axis_index('sh')
    new_slot = lax.rem(lens_ref[me], WINDOW)
    filled = jnp.minimum(lens_ref[me], WINDOW)
    block = math.gcd(BLOCK, size)
    count = size // block
    rows = pl.ds(0, block)

    @pl.when(filled < c0 + size)
    def _():
        zeros[...] = jnp.zeros_like(zeros)

    def empty(i):
        base = c0 + i * block
        return (base >= filled) & ((new_slot < base) | (new_slot >= base + block))

    def in_copies(i):
        slot = lax.rem(i, DEPTH)
        local = pl.ds(i * block, block)
        whole = pl.ds(c0 + i * block, block)
        views = (own.at[whole], near.at[whole], far0.at[local], far1.at[local])
        return [
            pltpu.make_async_copy(view, buf.at[slot, rows, :, me ^ j], in_sem.at[slot, j])
            for j, view in enumerate(views)
        ]

    def out_copy(i):
        slot = lax.rem(i, DEPTH)
        return pltpu.make_async_copy(buf.at[slot, rows], out.at[pl.ds(c0 + i * block, block)], out_sem.at[slot])

    def start_in(i):
        @pl.when(jnp.logical_not(empty(i)))
        def _():
            for copy in in_copies(i):
                copy.start()

    def finish(i):
        slot = lax.rem(i, DEPTH)
        base = c0 + i * block

        @pl.when(empty(i))
        def _():
            for part in range(block // ZEROS):
                pltpu.make_async_copy(zeros, out.at[pl.ds(base + part * ZEROS, ZEROS)], out_sem.at[slot]).start()

        @pl.when(jnp.logical_not(empty(i)))
        def _():
            for copy in in_copies(i):
                copy.wait()

            @pl.when(base + block > filled)
            def _():
                @pl.loop(jnp.maximum(filled - base, 0), block)
                def _(s):
                    buf[slot, s] = zeros[0]

            spot = new_slot - base

            @pl.when((spot >= 0) & (spot < block))
            def _():
                buf[slot, spot] = fresh_ref[...]

            out_copy(i).start()

    for i in range(min(DEPTH - 1, count)):
        start_in(jnp.int32(i))

    @pl.loop(0, count)
    def _(i):
        finish(i)
        ahead = i + DEPTH - 1

        @pl.when(ahead < count)
        def _():
            @pl.when(i >= 1)
            def _():
                out_copy(i - 1).wait()

            start_in(ahead)

    for i in range(max(count - DEPTH, 0), count):
        out_copy(jnp.int32(i)).wait()


def used_units(length):
    return (jnp.maximum(jnp.minimum(length, WINDOW) - LOW, 0) + UNIT - 1) // UNIT


def lane_counts(lens, half, lane):
    counts = []
    for g in range(LANES_OF_CUT):
        total = 2 * (used_units(lens(g, 2 * half)) + used_units(lens(g, 2 * half + 1)))
        counts.append((total + 3 - lane) // LANES_OF_CUT)
    return counts


def stream(count, depth, start_in, finish_in, start_out, wait_out):
    @pl.loop(0, jnp.minimum(count, depth - 1))
    def _(i):
        start_in(i)

    @pl.loop(0, count)
    def _(i):
        finish_in(i)
        start_out(i)
        ahead = i + depth - 1

        @pl.when(ahead < count)
        def _():
            @pl.when(i >= 1)
            def _():
                wait_out(i - 1)

            start_in(ahead)

    @pl.loop(jnp.maximum(count - depth, 0), count)
    def _(i):
        wait_out(i)


def pick(index, refs, action):
    for k, ref in enumerate(refs):
        @pl.when(index == k)
        def _():
            action(ref)


def deal_kernel(lens_ref, k_ref, v_ref, _, *refs):
    outs = refs[:LANES_OF_CUT]
    buf, other, in_sem, other_sem, out_sem = refs[LANES_OF_CUT:]
    depth = buf.shape[0]
    g = lax.axis_index('dp')
    row0 = 2 * (1 - lax.axis_index('sh') // 2)
    last = k_ref.shape[1] - UNIT
    counts = [used_units(lens_ref[row0 + c]) for c in (0, 1)]
    both = counts[0] + counts[1]

    def where(u):
        w = u - jnp.where(u >= both, both, 0)
        second = w >= counts[0]
        row = row0 + jnp.where(second, 1, 0)
        return u >= both, row, LOW + (w - jnp.where(second, counts[0], 0)) * UNIT, jnp.maximum(lens_ref[row] - WINDOW, 0)

    def in_copy(u, src, row, start):
        slot = lax.rem(u, depth)
        return pltpu.make_async_copy(src.at[row, pl.ds(start, UNIT)], buf.at[slot], in_sem.at[slot])

    def start_in(u):
        value, row, base, wrapped = where(u)
        start = jnp.where(base + UNIT <= wrapped, jnp.minimum(base + WINDOW, last), base)
        pick(jnp.where(value, 1, 0), (k_ref, v_ref), lambda src: in_copy(u, src, row, start).start())

    def finish_in(u):
        value, row, base, wrapped = where(u)
        slot = lax.rem(u, depth)
        in_copy(u, k_ref, row, 0).wait()

        @pl.when((base < wrapped) & (base + UNIT > wrapped))
        def _():
            def fetch(src):
                copy = pltpu.make_async_copy(src.at[row, pl.ds(jnp.minimum(base + WINDOW, last), UNIT)], other, other_sem)
                copy.start()
                copy.wait()

            pick(jnp.where(value, 1, 0), (k_ref, v_ref), fetch)

            @pl.loop(0, wrapped - base)
            def _(s):
                buf[slot, s] = other[s]

    def out_copy(u, out):
        slot = lax.rem(u, depth)
        return pltpu.make_async_copy(buf.at[slot], out.at[pl.ds(u // LANES_OF_CUT * UNIT, UNIT)], out_sem.at[slot])

    stream(2 * both, depth, start_in, finish_in,
           lambda u: pick(lax.rem(u, LANES_OF_CUT) ^ g, outs, lambda out: out_copy(u, out).start()),
           lambda u: out_copy(u, outs[0]).wait())


def compact_kernel(back, lens_ref, *refs):
    parts = LANES_OF_CUT * UPPER // PART
    sources = refs[:parts if back else LANES_OF_CUT]
    outs = refs[len(sources):len(sources) + (LANES_OF_CUT if back else parts)]
    buf, in_sem, out_sem = refs[-3:]
    depth = buf.shape[0]
    lane = lax.axis_index('dp')
    half = lax.axis_index('sh') // 2
    counts = lane_counts(lambda g, row: lens_ref[4 * g + row], half if back else 1 - half, lane)
    ends = [counts[0]]
    for count in counts[1:]:
        ends.append(ends[-1] + count)

    def spot(i):
        g = jnp.int32(0)
        first = jnp.int32(0)
        for k in range(LANES_OF_CUT - 1):
            g = jnp.where(i >= ends[k], k + 1, g)
            first = jnp.where(i >= ends[k], ends[k], first)
        container, dense = (g ^ lane, i - first), (i // PART, lax.rem(i, PART))
        return (dense, container) if back else (container, dense)

    def in_copy(i, src, at):
        slot = lax.rem(i, depth)
        return pltpu.make_async_copy(src.at[pl.ds(at * UNIT, UNIT)], buf.at[slot], in_sem.at[slot])

    def out_copy(i, out, at):
        slot = lax.rem(i, depth)
        return pltpu.make_async_copy(buf.at[slot], out.at[pl.ds(at * UNIT, UNIT)], out_sem.at[slot])

    def start_in(i):
        which, at = spot(i)[0]
        pick(which, sources, lambda src: in_copy(i, src, at).start())

    def start_out(i):
        which, at = spot(i)[1]
        pick(which, outs, lambda out: out_copy(i, out, at).start())

    stream(ends[-1], depth, start_in, lambda i: in_copy(i, sources[0], 0).wait(), start_out,
           lambda i: out_copy(i, outs[0], 0).wait())


def place_upper_kernel(values, lens_ref, fresh_ref, own, near, *refs):
    mine, others = refs[:LANES_OF_CUT], refs[LANES_OF_CUT:2 * LANES_OF_CUT]
    out, buf, zeros, in_sem, out_sem = refs[2 * LANES_OF_CUT + 1:]
    depth = buf.shape[0]
    g = lax.axis_index('dp')
    me = lax.axis_index('sh')
    core = lax.rem(me, 2)
    length = lens_ref[me]
    new_slot = lax.rem(length, WINDOW)
    filled = jnp.minimum(length, WINDOW)
    used = used_units(length)
    sibling = used_units(lens_ref[me ^ 1])
    start = jnp.where(core == 1, sibling, 0) + (used + sibling if values else 0)

    zeros[...] = jnp.zeros_like(zeros)

    def in_copy(b, j, view):
        slot = lax.rem(b, depth)
        return pltpu.make_async_copy(view, buf.at[slot, :, :, me ^ j], in_sem.at[slot, j])

    def start_in(b):
        @pl.when(b < used)
        def _():
            u = start + b
            at = pl.ds(u // LANES_OF_CUT * UNIT, UNIT)
            which = lax.rem(u, LANES_OF_CUT) ^ g
            here = pl.ds(LOW + b * UNIT, UNIT)
            in_copy(b, 0, own.at[here]).start()
            in_copy(b, 1, near.at[here]).start()
            pick(which, mine, lambda src: in_copy(b, 2, src.at[at]).start())
            pick(which, others, lambda src: in_copy(b, 3, src.at[at]).start())

    def finish_in(b):
        slot = lax.rem(b, depth)
        base = LOW + b * UNIT

        @pl.when(b < used)
        def _():
            for j in range(4):
                in_copy(b, j, own.at[pl.ds(0, UNIT)]).wait()

        spot = new_slot - base
        inside = (spot >= 0) & (spot < UNIT)

        @pl.when((base + UNIT > filled) & ((b < used) | inside))
        def _():
            @pl.loop(jnp.maximum(filled - base, 0), UNIT)
            def _(s):
                buf[slot, s] = zeros[0]

        @pl.when(inside)
        def _():
            buf[slot, spot] = fresh_ref[...]

    def out_copy(b):
        slot = lax.rem(b, depth)
        return pltpu.make_async_copy(buf.at[slot], out.at[pl.ds(LOW + b * UNIT, UNIT)], out_sem.at[slot])

    def start_out(b):
        slot = lax.rem(b, depth)
        base = LOW + b * UNIT
        blank = (b >= used) & ((new_slot < base) | (new_slot >= base + UNIT))

        @pl.when(blank)
        def _():
            for part in range(UNIT // ZEROS):
                pltpu.make_async_copy(zeros, out.at[pl.ds(base + part * ZEROS, ZEROS)], out_sem.at[slot]).start()

        @pl.when(jnp.logical_not(blank))
        def _():
            out_copy(b).start()

    stream(jnp.int32(UPPER), depth, start_in, finish_in, start_out, lambda b: out_copy(b).wait())


def local_call(kernel, scalars, vectors, arrays, outs, scratch, aliases, moved):
    hbm = pl.BlockSpec(memory_space=pltpu.HBM)
    return pl.pallas_call(
        kernel,
        out_shape=outs,
        in_specs=[pl.BlockSpec(memory_space=pltpu.SMEM)] * len(scalars) + [pl.BlockSpec(memory_space=pltpu.VMEM)] * len(vectors) + [hbm] * len(arrays),
        out_specs=jax.tree.map(lambda _: hbm, outs),
        scratch_shapes=scratch,
        input_output_aliases=aliases,
        compiler_params=pltpu.CompilerParams(vmem_limit_bytes=VMEM_BYTES),
        cost_estimate=pl.CostEstimate(flops=10 ** 9, bytes_accessed=moved, transcendentals=0),
    )(*scalars, *vectors, *arrays)


def deal(lengths, k_src, v_src, after):
    tile, dtype, depth = k_src.shape[2:], k_src.dtype, 2 * FLIGHT
    return local_call(
        deal_kernel, [lengths], [], [k_src, v_src, after],
        [jax.ShapeDtypeStruct((UPPER * UNIT,) + tile, dtype)] * LANES_OF_CUT,
        [pltpu.VMEM((depth, UNIT) + tile, dtype), pltpu.VMEM((UNIT,) + tile, dtype), pltpu.SemaphoreType.DMA((depth,)), pltpu.SemaphoreType.DMA, pltpu.SemaphoreType.DMA((depth,))],
        {}, 16 << 20)


def compact(every_length, arrays, back):
    tile, dtype, depth = arrays[0].shape[1:], arrays[0].dtype, 2 * FLIGHT
    many, size = (LANES_OF_CUT, UPPER) if back else (LANES_OF_CUT * UPPER // PART, PART)
    return local_call(
        functools.partial(compact_kernel, back), [every_length], [], arrays,
        [jax.ShapeDtypeStruct((size * UNIT,) + tile, dtype)] * many,
        [pltpu.VMEM((depth, UNIT) + tile, dtype), pltpu.SemaphoreType.DMA((depth,)), pltpu.SemaphoreType.DMA((depth,))],
        {}, 16 << 20)


def place_upper(values, lengths, fresh, own, near, mine, others, prev):
    halves, pair, lanes = own.shape[1:]
    depth = 8
    return local_call(
        functools.partial(place_upper_kernel, values), [lengths], [fresh], [own, near, *mine, *others, prev],
        jax.ShapeDtypeStruct(prev.shape, prev.dtype),
        [pltpu.VMEM((depth, UNIT, halves, 4, pair, lanes), own.dtype), pltpu.VMEM((ZEROS, halves, 4, pair, lanes), own.dtype), pltpu.SemaphoreType.DMA((depth, 4)), pltpu.SemaphoreType.DMA((depth,))],
        {4 + 2 * LANES_OF_CUT: 0}, 16 << 20)


def place(lengths, fresh, own, near, far0, far1, c0, prev):
    size = far0.shape[0]
    hbm = pl.BlockSpec(memory_space=pltpu.HBM)
    operands = [lengths, fresh, own, near, far0, far1]
    if prev is not None:
        operands.append(prev)
    halves, pair, lanes = own.shape[1:]
    return pl.pallas_call(
        functools.partial(place_kernel, c0, size, prev is not None),
        out_shape=jax.ShapeDtypeStruct((WINDOW, halves, 4, pair, lanes), own.dtype),
        in_specs=[pl.BlockSpec(memory_space=pltpu.SMEM), pl.BlockSpec(memory_space=pltpu.VMEM)] + [hbm] * (len(operands) - 2),
        out_specs=hbm,
        scratch_shapes=[
            pltpu.VMEM((DEPTH, BLOCK, halves, 4, pair, lanes), own.dtype),
            pltpu.VMEM((ZEROS, halves, 4, pair, lanes), own.dtype),
            pltpu.SemaphoreType.DMA((DEPTH, 4)),
            pltpu.SemaphoreType.DMA((DEPTH,)),
        ],
        input_output_aliases={} if prev is None else {6: 0},
        compiler_params=pltpu.CompilerParams(vmem_limit_bytes=VMEM_BYTES),
        cost_estimate=pl.CostEstimate(flops=10 ** 9, bytes_accessed=size * 8192, transcendentals=0),
    )(*operands)


def rotate(heads, positions):
    head_dim = heads.shape[-1]
    half_dim = head_dim // 2
    inv_freq = THETA ** (-2.0 * jnp.arange(half_dim, dtype=jnp.float32) / head_dim)
    angles = positions.astype(jnp.float32).reshape(positions.shape + (1,) * (heads.ndim - 1)) * inv_freq
    cos_part = jnp.cos(angles)
    sin_part = jnp.sin(angles)
    first_half = heads[..., :half_dim].astype(jnp.float32)
    second_half = heads[..., half_dim:].astype(jnp.float32)
    return jnp.concatenate([first_half * cos_part - second_half * sin_part, second_half * cos_part + first_half * sin_part], axis=-1).astype(jnp.bfloat16)


def normalize(residual, norm_gain):
    resid_f32 = residual.astype(jnp.float32)
    inv_rms = lax.rsqrt(jnp.mean(resid_f32 * resid_f32, axis=-1, keepdims=True) + EPS)
    return (resid_f32 * inv_rms * norm_gain.astype(jnp.float32)).astype(jnp.bfloat16)


def project(normed, weight):
    return jnp.dot(normed, weight, preferred_element_type=jnp.float32).astype(jnp.bfloat16)


def split_lanes(array):
    halves = array.shape[-1] // LANES
    return jnp.swapaxes(array.reshape(array.shape[:-1] + (halves, LANES)), -3, -2)


def attend_heads(q_heads, k_new, v_new, k_prefill, v_prefill, lengths):
    scale = q_heads.shape[-1] ** 0.5
    positions = jnp.arange(k_prefill.shape[1], dtype=jnp.int32)[None, :]
    live = (positions < lengths[:, None]) & (positions > lengths[:, None] - WINDOW)
    scores = jnp.einsum('rkgd,rwkd->rkgw', q_heads, k_prefill, preferred_element_type=jnp.float32) / scale
    scores = jnp.where(live[:, None, None, :], scores, -jnp.inf)
    new_score = jnp.sum(q_heads.astype(jnp.float32) * k_new.astype(jnp.float32)[:, :, None, :], axis=-1, keepdims=True) / scale
    top = jnp.maximum(jnp.max(scores, axis=-1, keepdims=True), new_score)
    exp_scores = jnp.exp(scores - top)
    new_exp = jnp.exp(new_score - top)
    total = jnp.sum(exp_scores, axis=-1, keepdims=True) + new_exp
    weights = (exp_scores / total).astype(jnp.bfloat16)
    new_weight = (new_exp / total).astype(jnp.bfloat16)
    mixed = jnp.einsum('rkgw,rwkd->rkgd', weights, v_prefill, preferred_element_type=jnp.float32)
    mixed = mixed + new_weight.astype(jnp.float32) * v_new.astype(jnp.float32)[:, :, None, :]
    return mixed.astype(jnp.bfloat16)


def solution(mesh):
    group = mesh.shape['sh']
    head_spec = P('dp', None, 'sh', None)
    row_spec = P(('dp', 'sh'))
    full_spec = P(None, None)

    def swap(array, j):
        return lax.ppermute(array, 'sh', [(i, i ^ j) for i in range(group)])

    def per_device(k_prefill, v_prefill, lengths, residual, norm_gain, w_query, w_key, w_value, w_out):
        kv_heads, head_dim = k_prefill.shape[2:]
        me = lax.axis_index('sh')
        by_row = jnp.arange(group, dtype=jnp.int32) ^ me

        all_resid = jnp.concatenate([residual] + [swap(residual, j) for j in range(1, group)], axis=0)
        all_resid = jnp.take(all_resid, by_row, axis=0)

        k_src, v_src = split_lanes(k_prefill), split_lanes(v_prefill)

        def build_far(src, chunks, i, after):
            return build(lengths, src, (2, 3), sum(chunks[:i]), chunks[i], after)

        def send_far(built):
            return [swap(a, j) for a, j in zip(built, (2, 3))]

        def shift(array, d):
            return lax.ppermute(array, 'dp', [(g, g ^ d) for g in range(LANES_OF_CUT)])

        every_length = jnp.stack([lengths] + [shift(lengths, d) for d in range(1, LANES_OF_CUT)])
        every_length = jnp.take(every_length, jnp.arange(LANES_OF_CUT, dtype=jnp.int32) ^ lax.axis_index('dp'), axis=0).reshape(-1)

        k_first = build_far(k_src, K_CHUNKS, 0, lengths)
        k_far = [send_far(k_first)]
        dealt = deal(lengths, k_src, v_src, k_first[0])
        k_second = build_far(k_src, K_CHUNKS, 1, dealt[0])
        dealt = [dealt[0]] + [shift(a, d + 1) for d, a in enumerate(dealt[1:])]
        k_far.append(send_far(k_second))
        v_built = []
        for i in range(len(V_CHUNKS)):
            v_built.append(build_far(v_src, V_CHUNKS, i, (k_second if i == 0 else v_built[-1])[0]))

        normed = normalize(all_resid, norm_gain)
        kv_width = kv_heads * head_dim
        q_width = w_query.shape[1] // group
        q_heads = project(normed, lax.dynamic_slice_in_dim(w_query, me * q_width, q_width, axis=1))
        q_heads = rotate(q_heads.reshape(group, kv_heads, q_width // kv_width, head_dim), lengths)
        k_new = project(normed, lax.dynamic_slice_in_dim(w_key, me * kv_width, kv_width, axis=1))
        v_new = project(normed, lax.dynamic_slice_in_dim(w_value, me * kv_width, kv_width, axis=1))
        k_new = rotate(k_new.reshape(group, kv_heads, head_dim), lengths)
        v_new = v_new.reshape(group, kv_heads, head_dim)
        mixed = attend_heads(q_heads, k_new, v_new, k_prefill, v_prefill, lengths).reshape(group, q_width)
        mixed = jnp.concatenate([mixed, k_new.reshape(group, kv_width), v_new.reshape(group, kv_width)], axis=1)
        mixed = jnp.take(mixed, by_row, axis=0)
        mine = [mixed[:1]] + [swap(mixed[j:j + 1], j) for j in range(1, group)]

        parts = compact(every_length, dealt, False)
        parts, v_built = lax.optimization_barrier((parts, v_built))
        by_group = every_length.reshape(LANES_OF_CUT, group)
        level = jnp.int32(0)
        for half in range(2):
            for lane in range(LANES_OF_CUT):
                level = jnp.maximum(level, sum(lane_counts(lambda g, row: by_group[g, row], half, lane)))

        def cross(count):
            def branch(*arrays):
                return [lax.ppermute(a, 'sh', [(i, i ^ 2) for i in range(group)]) if i < count else a for i, a in enumerate(arrays)]

            return branch

        parts = lax.switch((level + PART - 1) // PART, [cross(count) for count in range(len(parts) + 1)], *parts)

        v_far = [send_far(built) for built in v_built]
        dealt = compact(every_length, parts, True)
        dealt = [dealt[0]] + [shift(a, d + 1) for d, a in enumerate(dealt[1:])]
        others = [swap(a, 1) for a in dealt]
        k_own, k_near = build(lengths, k_src, (0, 1), 0, WINDOW, parts[0])
        k_near = swap(k_near, 1)
        v_own, v_near = build(lengths, v_src, (0, 1), 0, WINDOW, parts[0])
        v_near = swap(v_near, 1)

        mine = jnp.take(jnp.concatenate(mine, axis=0), by_row, axis=0)
        attn_out = mine[:, :q_width].reshape(1, group * q_width)
        resid_out = (residual.astype(jnp.float32) + jnp.dot(attn_out, w_out, preferred_element_type=jnp.float32)).astype(jnp.bfloat16)

        k_fresh = mine[:, q_width:q_width + kv_width].reshape(1, group * kv_heads, head_dim)
        v_fresh = mine[:, q_width + kv_width:].reshape(1, group * kv_heads, head_dim)

        def cache(fresh, own, near, far, values):
            fresh = split_lanes(fresh[0])
            fresh = fresh.reshape(fresh.shape[0], group, kv_heads, LANES)
            out, c0 = None, 0
            for far0, far1 in far:
                if values and c0 + far0.shape[0] == LOW:
                    out = place_upper(values, lengths, fresh, own, near, dealt, others, out)
                out = place(lengths, fresh, own, near, far0, far1, c0, out)
                c0 += far0.shape[0]
            if not values:
                out = place_upper(values, lengths, fresh, own, near, dealt, others, out)
            return jnp.transpose(out, (0, 2, 3, 1, 4)).reshape(1, WINDOW, group * kv_heads, head_dim)

        return resid_out, cache(k_fresh, k_own, k_near, k_far, False), cache(v_fresh, v_own, v_near, v_far, True)

    return jax.shard_map(per_device, mesh=mesh, in_specs=(head_spec, head_spec, P('dp'), P(('dp', 'sh'), None), P(None), full_spec, full_spec, full_spec, full_spec), out_specs=(P(('dp', 'sh'), None), row_spec, row_spec), check_vma=False)
```

```python
import functools
import math

import jax
import jax.numpy as jnp
from jax import lax
from jax.experimental import pallas as pl
from jax.experimental.pallas import tpu as pltpu
from jax.sharding import PartitionSpec as P


WINDOW = 4096
THETA = 10000.0
EPS = 1e-5
LANES = 128
BLOCK = 256
DEPTH = 6
FLIGHT = 16
ZEROS = 32
VMEM_BYTES = 67043328
LOW = 2560
K_CHUNKS = (512, 2048)
V_CHUNKS = (1792, 512, 256)
UNIT = 128
UPPER = (WINDOW - LOW) // UNIT
LANES_OF_CUT = 4
PART = 3


def build_kernel(partners, c0, lens_ref, src_ref, _, *refs):
    ways = len(partners)
    outs = refs[:ways]
    buf, other, in_sem, other_sem, out_sem = refs[ways:]
    me = lax.axis_index('sh')
    size = outs[0].shape[0]
    block = math.gcd(BLOCK, size)
    total = size // block * ways
    last = src_ref.shape[1] - block
    rows = pl.ds(0, block)

    def where(i):
        row = me ^ partners[0]
        for p, j in enumerate(partners[1:]):
            row = jnp.where(lax.rem(i, ways) == p + 1, me ^ j, row)
        return row, c0 + i // ways * block, jnp.maximum(lens_ref[row] - WINDOW, 0)

    def in_copy(i, row, start):
        slot = lax.rem(i, FLIGHT)
        return pltpu.make_async_copy(src_ref.at[row, pl.ds(start, block)], buf.at[slot, rows], in_sem.at[slot])

    def other_copy(row, start):
        return pltpu.make_async_copy(src_ref.at[row, pl.ds(start, block)], other.at[rows], other_sem)

    def out_copy(i, out):
        slot = lax.rem(i, FLIGHT)
        return pltpu.make_async_copy(buf.at[slot, rows], out.at[pl.ds(i // ways * block, block)], out_sem.at[slot])

    def start_in(i):
        row, base, wrapped = where(i)
        in_copy(i, row, jnp.where(base + block <= wrapped, jnp.minimum(base + WINDOW, last), base)).start()

    def finish(i):
        row, base, wrapped = where(i)
        slot = lax.rem(i, FLIGHT)
        in_copy(i, row, 0).wait()

        @pl.when((base < wrapped) & (base + block > wrapped))
        def _():
            copy = other_copy(row, jnp.minimum(base + WINDOW, last))
            copy.start()
            copy.wait()

            @pl.loop(0, wrapped - base)
            def _(s):
                buf[slot, s] = other[s]

        for p, out in enumerate(outs):
            @pl.when(lax.rem(i, ways) == p)
            def _():
                out_copy(i, out).start()

    @pl.loop(0, min(FLIGHT - 1, total))
    def _(i):
        start_in(i)

    @pl.loop(0, total)
    def _(i):
        finish(i)
        ahead = i + FLIGHT - 1

        @pl.when(ahead < total)
        def _():
            @pl.when(i >= 1)
            def _():
                out_copy(i - 1, outs[0]).wait()

            start_in(ahead)

    @pl.loop(max(total - FLIGHT, 0), total)
    def _(i):
        out_copy(i, outs[0]).wait()


def build(lengths, src, partners, c0, size, after):
    tile = src.shape[2:]
    return pl.pallas_call(
        functools.partial(build_kernel, partners, c0),
        out_shape=[jax.ShapeDtypeStruct((size,) + tile, src.dtype) for _ in partners],
        in_specs=[pl.BlockSpec(memory_space=pltpu.SMEM), pl.BlockSpec(memory_space=pltpu.HBM), pl.BlockSpec(memory_space=pl.ANY)],
        out_specs=[pl.BlockSpec(memory_space=pltpu.HBM)] * len(partners),
        scratch_shapes=[
            pltpu.VMEM((FLIGHT, BLOCK) + tile, src.dtype),
            pltpu.VMEM((BLOCK,) + tile, src.dtype),
            pltpu.SemaphoreType.DMA((FLIGHT,)),
            pltpu.SemaphoreType.DMA,
            pltpu.SemaphoreType.DMA((FLIGHT,)),
        ],
        compiler_params=pltpu.CompilerParams(vmem_limit_bytes=VMEM_BYTES),
        cost_estimate=pl.CostEstimate(flops=10 ** 9, bytes_accessed=size * 4096, transcendentals=0),
    )(lengths, src, after)


def place_kernel(c0, size, has_prev, lens_ref, fresh_ref, own, near, far0, far1, *refs):
    out = refs[1] if has_prev else refs[0]
    buf, zeros, in_sem, out_sem = refs[-4:]
    me = lax.axis_index('sh')
    new_slot = lax.rem(lens_ref[me], WINDOW)
    filled = jnp.minimum(lens_ref[me], WINDOW)
    block = math.gcd(BLOCK, size)
    count = size // block
    rows = pl.ds(0, block)

    @pl.when(filled < c0 + size)
    def _():
        zeros[...] = jnp.zeros_like(zeros)

    def empty(i):
        base = c0 + i * block
        return (base >= filled) & ((new_slot < base) | (new_slot >= base + block))

    def in_copies(i):
        slot = lax.rem(i, DEPTH)
        local = pl.ds(i * block, block)
        whole = pl.ds(c0 + i * block, block)
        views = (own.at[whole], near.at[whole], far0.at[local], far1.at[local])
        return [
            pltpu.make_async_copy(view, buf.at[slot, rows, :, me ^ j], in_sem.at[slot, j])
            for j, view in enumerate(views)
        ]

    def out_copy(i):
        slot = lax.rem(i, DEPTH)
        return pltpu.make_async_copy(buf.at[slot, rows], out.at[pl.ds(c0 + i * block, block)], out_sem.at[slot])

    def start_in(i):
        @pl.when(jnp.logical_not(empty(i)))
        def _():
            for copy in in_copies(i):
                copy.start()

    def finish(i):
        slot = lax.rem(i, DEPTH)
        base = c0 + i * block

        @pl.when(empty(i))
        def _():
            for part in range(block // ZEROS):
                pltpu.make_async_copy(zeros, out.at[pl.ds(base + part * ZEROS, ZEROS)], out_sem.at[slot]).start()

        @pl.when(jnp.logical_not(empty(i)))
        def _():
            for copy in in_copies(i):
                copy.wait()

            @pl.when(base + block > filled)
            def _():
                @pl.loop(jnp.maximum(filled - base, 0), block)
                def _(s):
                    buf[slot, s] = zeros[0]

            spot = new_slot - base

            @pl.when((spot >= 0) & (spot < block))
            def _():
                buf[slot, spot] = fresh_ref[...]

            out_copy(i).start()

    for i in range(min(DEPTH - 1, count)):
        start_in(jnp.int32(i))

    @pl.loop(0, count)
    def _(i):
        finish(i)
        ahead = i + DEPTH - 1

        @pl.when(ahead < count)
        def _():
            @pl.when(i >= 1)
            def _():
                out_copy(i - 1).wait()

            start_in(ahead)

    for i in range(max(count - DEPTH, 0), count):
        out_copy(jnp.int32(i)).wait()


def used_units(length):
    return (jnp.maximum(jnp.minimum(length, WINDOW) - LOW, 0) + UNIT - 1) >> 7


def lane_counts(lens, half, lane):
    counts = []
    for g in range(LANES_OF_CUT):
        total = 2 * (used_units(lens(g, 2 * half)) + used_units(lens(g, 2 * half + 1)))
        counts.append((total + 3 - lane) // LANES_OF_CUT)
    return counts


def stream(count, depth, start_in, finish_in, start_out, wait_out):
    @pl.loop(0, jnp.minimum(count, depth - 1))
    def _(i):
        start_in(i)

    @pl.loop(0, count)
    def _(i):
        finish_in(i)
        start_out(i)
        ahead = i + depth - 1

        @pl.when(ahead < count)
        def _():
            @pl.when(i >= 1)
            def _():
                wait_out(i - 1)

            start_in(ahead)

    @pl.loop(jnp.maximum(count - depth, 0), count)
    def _(i):
        wait_out(i)


def pick(index, refs, action):
    for k, ref in enumerate(refs):
        @pl.when(index == k)
        def _():
            action(ref)


def deal_kernel(lens_ref, k_ref, v_ref, _, *refs):
    outs = refs[:LANES_OF_CUT]
    buf, other, in_sem, other_sem, out_sem = refs[LANES_OF_CUT:]
    depth = buf.shape[0]
    g = lax.axis_index('dp')
    row0 = 2 * (1 - lax.axis_index('sh') // 2)
    last = k_ref.shape[1] - UNIT
    counts = [used_units(lens_ref[row0 + c]) for c in (0, 1)]
    both = counts[0] + counts[1]

    def where(u):
        w = u - jnp.where(u >= both, both, 0)
        second = w >= counts[0]
        row = row0 + jnp.where(second, 1, 0)
        return u >= both, row, LOW + (w - jnp.where(second, counts[0], 0)) * UNIT, jnp.maximum(lens_ref[row] - WINDOW, 0)

    def in_copy(u, src, row, start):
        slot = lax.rem(u, depth)
        return pltpu.make_async_copy(src.at[row, pl.ds(start, UNIT)], buf.at[slot], in_sem.at[slot])

    def start_in(u):
        value, row, base, wrapped = where(u)
        start = jnp.where(base + UNIT <= wrapped, jnp.minimum(base + WINDOW, last), base)
        pick(jnp.where(value, 1, 0), (k_ref, v_ref), lambda src: in_copy(u, src, row, start).start())

    def finish_in(u):
        value, row, base, wrapped = where(u)
        slot = lax.rem(u, depth)
        in_copy(u, k_ref, row, 0).wait()

        @pl.when((base < wrapped) & (base + UNIT > wrapped))
        def _():
            def fetch(src):
                copy = pltpu.make_async_copy(src.at[row, pl.ds(jnp.minimum(base + WINDOW, last), UNIT)], other, other_sem)
                copy.start()
                copy.wait()

            pick(jnp.where(value, 1, 0), (k_ref, v_ref), fetch)

            @pl.loop(0, wrapped - base)
            def _(s):
                buf[slot, s] = other[s]

    def out_copy(u, out):
        slot = lax.rem(u, depth)
        return pltpu.make_async_copy(buf.at[slot], out.at[pl.ds(u // LANES_OF_CUT * UNIT, UNIT)], out_sem.at[slot])

    stream(2 * both, depth, start_in, finish_in,
           lambda u: pick(lax.rem(u, LANES_OF_CUT) ^ g, outs, lambda out: out_copy(u, out).start()),
           lambda u: out_copy(u, outs[0]).wait())


def compact_kernel(back, lens_ref, *refs):
    parts = LANES_OF_CUT * UPPER // PART
    sources = refs[:parts if back else LANES_OF_CUT]
    outs = refs[len(sources):len(sources) + (LANES_OF_CUT if back else parts)]
    buf, in_sem, out_sem = refs[-3:]
    depth = buf.shape[0]
    lane = lax.axis_index('dp')
    half = lax.axis_index('sh') // 2
    counts = lane_counts(lambda g, row: lens_ref[4 * g + row], half if back else 1 - half, lane)
    ends = [counts[0]]
    for count in counts[1:]:
        ends.append(ends[-1] + count)

    def spot(i):
        g = jnp.int32(0)
        first = jnp.int32(0)
        for k in range(LANES_OF_CUT - 1):
            g = jnp.where(i >= ends[k], k + 1, g)
            first = jnp.where(i >= ends[k], ends[k], first)
        container, dense = (g ^ lane, i - first), (i // PART, lax.rem(i, PART))
        return (dense, container) if back else (container, dense)

    def in_copy(i, src, at):
        slot = lax.rem(i, depth)
        return pltpu.make_async_copy(src.at[pl.ds(at * UNIT, UNIT)], buf.at[slot], in_sem.at[slot])

    def out_copy(i, out, at):
        slot = lax.rem(i, depth)
        return pltpu.make_async_copy(buf.at[slot], out.at[pl.ds(at * UNIT, UNIT)], out_sem.at[slot])

    def start_in(i):
        which, at = spot(i)[0]
        pick(which, sources, lambda src: in_copy(i, src, at).start())

    def start_out(i):
        which, at = spot(i)[1]
        pick(which, outs, lambda out: out_copy(i, out, at).start())

    stream(ends[-1], depth, start_in, lambda i: in_copy(i, sources[0], 0).wait(), start_out,
           lambda i: out_copy(i, outs[0], 0).wait())


def place_upper_kernel(values, lens_ref, fresh_ref, own, near, *refs):
    mine, others = refs[:LANES_OF_CUT], refs[LANES_OF_CUT:2 * LANES_OF_CUT]
    out, buf, zeros, in_sem, out_sem = refs[2 * LANES_OF_CUT + 1:]
    depth = buf.shape[0]
    g = lax.axis_index('dp')
    me = lax.axis_index('sh')
    core = lax.rem(me, 2)
    length = lens_ref[me]
    new_slot = lax.rem(length, WINDOW)
    filled = jnp.minimum(length, WINDOW)
    used = used_units(length)
    sibling = used_units(lens_ref[me ^ 1])
    start = jnp.where(core == 1, sibling, 0) + (used + sibling if values else 0)

    zeros[...] = jnp.zeros_like(zeros)

    def in_copy(b, j, view):
        slot = lax.rem(b, depth)
        return pltpu.make_async_copy(view, buf.at[slot, :, :, me ^ j], in_sem.at[slot, j])

    def start_in(b):
        @pl.when(b < used)
        def _():
            u = start + b
            at = pl.ds(u // LANES_OF_CUT * UNIT, UNIT)
            which = lax.rem(u, LANES_OF_CUT) ^ g
            here = pl.ds(LOW + b * UNIT, UNIT)
            in_copy(b, 0, own.at[here]).start()
            in_copy(b, 1, near.at[here]).start()
            pick(which, mine, lambda src: in_copy(b, 2, src.at[at]).start())
            pick(which, others, lambda src: in_copy(b, 3, src.at[at]).start())

    def finish_in(b):
        slot = lax.rem(b, depth)
        base = LOW + b * UNIT

        @pl.when(b < used)
        def _():
            for j in range(4):
                in_copy(b, j, own.at[pl.ds(0, UNIT)]).wait()

        spot = new_slot - base
        inside = (spot >= 0) & (spot < UNIT)

        @pl.when((base + UNIT > filled) & ((b < used) | inside))
        def _():
            @pl.loop(jnp.maximum(filled - base, 0), UNIT)
            def _(s):
                buf[slot, s] = zeros[0]

        @pl.when(inside)
        def _():
            buf[slot, spot] = fresh_ref[...]

    def out_copy(b):
        slot = lax.rem(b, depth)
        return pltpu.make_async_copy(buf.at[slot], out.at[pl.ds(LOW + b * UNIT, UNIT)], out_sem.at[slot])

    def start_out(b):
        slot = lax.rem(b, depth)
        base = LOW + b * UNIT
        blank = (b >= used) & ((new_slot < base) | (new_slot >= base + UNIT))

        @pl.when(blank)
        def _():
            for part in range(UNIT // ZEROS):
                pltpu.make_async_copy(zeros, out.at[pl.ds(base + part * ZEROS, ZEROS)], out_sem.at[slot]).start()

        @pl.when(jnp.logical_not(blank))
        def _():
            out_copy(b).start()

    stream(jnp.int32(UPPER), depth, start_in, finish_in, start_out, lambda b: out_copy(b).wait())


def local_call(kernel, scalars, vectors, arrays, outs, scratch, aliases, moved):
    hbm = pl.BlockSpec(memory_space=pltpu.HBM)
    return pl.pallas_call(
        kernel,
        out_shape=outs,
        in_specs=[pl.BlockSpec(memory_space=pltpu.SMEM)] * len(scalars) + [pl.BlockSpec(memory_space=pltpu.VMEM)] * len(vectors) + [hbm] * len(arrays),
        out_specs=jax.tree.map(lambda _: hbm, outs),
        scratch_shapes=scratch,
        input_output_aliases=aliases,
        compiler_params=pltpu.CompilerParams(vmem_limit_bytes=VMEM_BYTES),
        cost_estimate=pl.CostEstimate(flops=10 ** 9, bytes_accessed=moved, transcendentals=0),
    )(*scalars, *vectors, *arrays)


def deal(lengths, k_src, v_src, after):
    tile, dtype, depth = k_src.shape[2:], k_src.dtype, 2 * FLIGHT
    return local_call(
        deal_kernel, [lengths], [], [k_src, v_src, after],
        [jax.ShapeDtypeStruct((UPPER * UNIT,) + tile, dtype)] * LANES_OF_CUT,
        [pltpu.VMEM((depth, UNIT) + tile, dtype), pltpu.VMEM((UNIT,) + tile, dtype), pltpu.SemaphoreType.DMA((depth,)), pltpu.SemaphoreType.DMA, pltpu.SemaphoreType.DMA((depth,))],
        {}, 16 << 20)


def compact(every_length, arrays, back):
    tile, dtype, depth = arrays[0].shape[1:], arrays[0].dtype, 2 * FLIGHT
    many, size = (LANES_OF_CUT, UPPER) if back else (LANES_OF_CUT * UPPER // PART, PART)
    return local_call(
        functools.partial(compact_kernel, back), [every_length], [], arrays,
        [jax.ShapeDtypeStruct((size * UNIT,) + tile, dtype)] * many,
        [pltpu.VMEM((depth, UNIT) + tile, dtype), pltpu.SemaphoreType.DMA((depth,)), pltpu.SemaphoreType.DMA((depth,))],
        {}, 16 << 20)


def place_upper(values, lengths, fresh, own, near, mine, others, prev):
    halves, pair, lanes = own.shape[1:]
    depth = 8
    return local_call(
        functools.partial(place_upper_kernel, values), [lengths], [fresh], [own, near, *mine, *others, prev],
        jax.ShapeDtypeStruct(prev.shape, prev.dtype),
        [pltpu.VMEM((depth, UNIT, halves, 4, pair, lanes), own.dtype), pltpu.VMEM((ZEROS, halves, 4, pair, lanes), own.dtype), pltpu.SemaphoreType.DMA((depth, 4)), pltpu.SemaphoreType.DMA((depth,))],
        {4 + 2 * LANES_OF_CUT: 0}, 16 << 20)


def place(lengths, fresh, own, near, far0, far1, c0, prev):
    size = far0.shape[0]
    hbm = pl.BlockSpec(memory_space=pltpu.HBM)
    operands = [lengths, fresh, own, near, far0, far1]
    if prev is not None:
        operands.append(prev)
    halves, pair, lanes = own.shape[1:]
    return pl.pallas_call(
        functools.partial(place_kernel, c0, size, prev is not None),
        out_shape=jax.ShapeDtypeStruct((WINDOW, halves, 4, pair, lanes), own.dtype),
        in_specs=[pl.BlockSpec(memory_space=pltpu.SMEM), pl.BlockSpec(memory_space=pltpu.VMEM)] + [hbm] * (len(operands) - 2),
        out_specs=hbm,
        scratch_shapes=[
            pltpu.VMEM((DEPTH, BLOCK, halves, 4, pair, lanes), own.dtype),
            pltpu.VMEM((ZEROS, halves, 4, pair, lanes), own.dtype),
            pltpu.SemaphoreType.DMA((DEPTH, 4)),
            pltpu.SemaphoreType.DMA((DEPTH,)),
        ],
        input_output_aliases={} if prev is None else {6: 0},
        compiler_params=pltpu.CompilerParams(vmem_limit_bytes=VMEM_BYTES),
        cost_estimate=pl.CostEstimate(flops=10 ** 9, bytes_accessed=size * 8192, transcendentals=0),
    )(*operands)


def rotate(heads, positions):
    head_dim = heads.shape[-1]
    half_dim = head_dim // 2
    inv_freq = THETA ** (-2.0 * jnp.arange(half_dim, dtype=jnp.float32) / head_dim)
    angles = positions.astype(jnp.float32).reshape(positions.shape + (1,) * (heads.ndim - 1)) * inv_freq
    cos_part = jnp.cos(angles)
    sin_part = jnp.sin(angles)
    first_half = heads[..., :half_dim].astype(jnp.float32)
    second_half = heads[..., half_dim:].astype(jnp.float32)
    return jnp.concatenate([first_half * cos_part - second_half * sin_part, second_half * cos_part + first_half * sin_part], axis=-1).astype(jnp.bfloat16)


def normalize(residual, norm_gain):
    resid_f32 = residual.astype(jnp.float32)
    inv_rms = lax.rsqrt(jnp.mean(resid_f32 * resid_f32, axis=-1, keepdims=True) + EPS)
    return (resid_f32 * inv_rms * norm_gain.astype(jnp.float32)).astype(jnp.bfloat16)


def project(normed, weight):
    return jnp.dot(normed, weight, preferred_element_type=jnp.float32).astype(jnp.bfloat16)


def split_lanes(array):
    halves = array.shape[-1] // LANES
    return jnp.swapaxes(array.reshape(array.shape[:-1] + (halves, LANES)), -3, -2)


def attend_heads(q_heads, k_new, v_new, k_prefill, v_prefill, lengths):
    scale = q_heads.shape[-1] ** 0.5
    positions = jnp.arange(k_prefill.shape[1], dtype=jnp.int32)[None, :]
    live = (positions < lengths[:, None]) & (positions > lengths[:, None] - WINDOW)
    scores = jnp.einsum('rkgd,rwkd->rkgw', q_heads, k_prefill, preferred_element_type=jnp.float32) / scale
    scores = jnp.where(live[:, None, None, :], scores, -jnp.inf)
    new_score = jnp.sum(q_heads.astype(jnp.float32) * k_new.astype(jnp.float32)[:, :, None, :], axis=-1, keepdims=True) / scale
    top = jnp.maximum(jnp.max(scores, axis=-1, keepdims=True), new_score)
    exp_scores = jnp.exp(scores - top)
    new_exp = jnp.exp(new_score - top)
    total = jnp.sum(exp_scores, axis=-1, keepdims=True) + new_exp
    weights = (exp_scores / total).astype(jnp.bfloat16)
    new_weight = (new_exp / total).astype(jnp.bfloat16)
    mixed = jnp.einsum('rkgw,rwkd->rkgd', weights, v_prefill, preferred_element_type=jnp.float32)
    mixed = mixed + new_weight.astype(jnp.float32) * v_new.astype(jnp.float32)[:, :, None, :]
    return mixed.astype(jnp.bfloat16)


def solution(mesh):
    group = mesh.shape['sh']
    head_spec = P('dp', None, 'sh', None)
    row_spec = P(('dp', 'sh'))
    full_spec = P(None, None)

    def swap(array, j):
        return lax.ppermute(array, 'sh', [(i, i ^ j) for i in range(group)])

    def per_device(k_prefill, v_prefill, lengths, residual, norm_gain, w_query, w_key, w_value, w_out):
        kv_heads, head_dim = k_prefill.shape[2:]
        me = lax.axis_index('sh')
        by_row = jnp.arange(group, dtype=jnp.int32) ^ me

        all_resid = jnp.concatenate([residual] + [swap(residual, j) for j in range(1, group)], axis=0)
        all_resid = jnp.take(all_resid, by_row, axis=0)

        k_src, v_src = split_lanes(k_prefill), split_lanes(v_prefill)

        def build_far(src, chunks, i, after):
            return build(lengths, src, (2, 3), sum(chunks[:i]), chunks[i], after)

        def send_far(built):
            return [swap(a, j) for a, j in zip(built, (2, 3))]

        def shift(array, d):
            return lax.ppermute(array, 'dp', [(g, g ^ d) for g in range(LANES_OF_CUT)])

        every_length = jnp.stack([lengths] + [shift(lengths, d) for d in range(1, LANES_OF_CUT)])
        every_length = jnp.take(every_length, jnp.arange(LANES_OF_CUT, dtype=jnp.int32) ^ lax.axis_index('dp'), axis=0).reshape(-1)

        k_first = build_far(k_src, K_CHUNKS, 0, lengths)
        k_far = [send_far(k_first)]
        dealt = deal(lengths, k_src, v_src, k_first[0])
        k_second = build_far(k_src, K_CHUNKS, 1, dealt[0])
        dealt = [dealt[0]] + [shift(a, d + 1) for d, a in enumerate(dealt[1:])]
        k_far.append(send_far(k_second))
        v_built = []
        for i in range(len(V_CHUNKS)):
            v_built.append(build_far(v_src, V_CHUNKS, i, (k_second if i == 0 else v_built[-1])[0]))

        normed = normalize(all_resid, norm_gain)
        kv_width = kv_heads * head_dim
        q_width = w_query.shape[1] // group
        q_heads = project(normed, lax.dynamic_slice_in_dim(w_query, me * q_width, q_width, axis=1))
        q_heads = rotate(q_heads.reshape(group, kv_heads, q_width // kv_width, head_dim), lengths)
        k_new = project(normed, lax.dynamic_slice_in_dim(w_key, me * kv_width, kv_width, axis=1))
        v_new = project(normed, lax.dynamic_slice_in_dim(w_value, me * kv_width, kv_width, axis=1))
        k_new = rotate(k_new.reshape(group, kv_heads, head_dim), lengths)
        v_new = v_new.reshape(group, kv_heads, head_dim)
        mixed = attend_heads(q_heads, k_new, v_new, k_prefill, v_prefill, lengths).reshape(group, q_width)
        mixed = jnp.concatenate([mixed, k_new.reshape(group, kv_width), v_new.reshape(group, kv_width)], axis=1)
        mixed = jnp.take(mixed, by_row, axis=0)
        mine = [mixed[:1]] + [swap(mixed[j:j + 1], j) for j in range(1, group)]

        parts = compact(every_length, dealt, False)
        parts, v_built = lax.optimization_barrier((parts, v_built))
        by_group = every_length.reshape(LANES_OF_CUT, group)
        totals = used_units(by_group).reshape(LANES_OF_CUT, 2, 2).sum(-1) * 2
        lanes = jnp.arange(LANES_OF_CUT, dtype=jnp.int32)
        level = jnp.max(jnp.sum(jnp.right_shift(totals[:, :, None] + (LANES_OF_CUT - 1 - lanes), 2), axis=0))

        def cross(count):
            def branch(*arrays):
                return [lax.ppermute(a, 'sh', [(i, i ^ 2) for i in range(group)]) if i < count else a for i, a in enumerate(arrays)]

            return branch

        parts = lax.switch(lax.div(level + PART - 1, PART), [cross(count) for count in range(len(parts) + 1)], *parts)

        v_far = [send_far(built) for built in v_built]
        dealt = compact(every_length, parts, True)
        dealt = [dealt[0]] + [shift(a, d + 1) for d, a in enumerate(dealt[1:])]
        others = [swap(a, 1) for a in dealt]
        k_own, k_near = build(lengths, k_src, (0, 1), 0, WINDOW, parts[0])
        k_near = swap(k_near, 1)
        v_own, v_near = build(lengths, v_src, (0, 1), 0, WINDOW, parts[0])
        v_near = swap(v_near, 1)

        mine = jnp.take(jnp.concatenate(mine, axis=0), by_row, axis=0)
        attn_out = mine[:, :q_width].reshape(1, group * q_width)
        resid_out = (residual.astype(jnp.float32) + jnp.dot(attn_out, w_out, preferred_element_type=jnp.float32)).astype(jnp.bfloat16)

        k_fresh = mine[:, q_width:q_width + kv_width].reshape(1, group * kv_heads, head_dim)
        v_fresh = mine[:, q_width + kv_width:].reshape(1, group * kv_heads, head_dim)

        def cache(fresh, own, near, far, values):
            fresh = split_lanes(fresh[0])
            fresh = fresh.reshape(fresh.shape[0], group, kv_heads, LANES)
            out, c0 = None, 0
            for far0, far1 in far:
                if values and c0 == V_CHUNKS[0]:
                    out = place_upper(values, lengths, fresh, own, near, dealt, others, out)
                out = place(lengths, fresh, own, near, far0, far1, c0, out)
                c0 += far0.shape[0]
            if not values:
                out = place_upper(values, lengths, fresh, own, near, dealt, others, out)
            return jnp.transpose(out, (0, 2, 3, 1, 4)).reshape(1, WINDOW, group * kv_heads, head_dim)

        return resid_out, cache(k_fresh, k_own, k_near, k_far, False), cache(v_fresh, v_own, v_near, v_far, True)

    return jax.shard_map(per_device, mesh=mesh, in_specs=(head_spec, head_spec, P('dp'), P(('dp', 'sh'), None), P(None), full_spec, full_spec, full_spec, full_spec), out_specs=(P(('dp', 'sh'), None), row_spec, row_spec), check_vma=False)
```
